32 devices in a mesh: dp: 8 (over y, x, core), mp: 4 (over z).
Axes of the slice: x: 2, y: 2, z: 4, core: 2. Of those that a mesh axis runs over, the one named last changes fastest.
Arguments:
- activations: bfloat16 [4096, 8192], P('dp', 'mp'), may hold values from -6 to 6
- out_grads: bfloat16 [4096, 1024], P('dp'), may hold values from -0.06591797 to 0.06591797
- projector: bfloat16 [8192, 512], P('mp'), may hold values from -0.0625 to 0.0625
- weight: float32 [8192, 1024], P('mp'), may hold values from -0.00024 to 0.00024
- first_moment: float32 [512, 1024], P('dp', 'mp'), may hold values from -0.6 to 0.6
- second_moment: float32 [512, 1024], P('dp', 'mp'), may hold values from 0.0003 to 0.003
Outputs:
- new_weight: float32 [8192, 1024], P('mp')
- update: bfloat16 [8192, 1024], P('mp')
- first_new: float32 [512, 1024], P('dp', 'mp')
- second_new: float32 [512, 1024], P('dp', 'mp')
The draws below stay inside these ranges and needn't reach their ends.
All inputs are finite; a program needn't handle non-finite values.
Results may differ from the reference program's by a relative error of at most 0.008.
Values may be sent and summed in bfloat16 or wider, within the bound.
No kernel may reach another device: no remote copies, remote signals or barrier semaphores. Data moves between devices by JAX's collectives and lax.ppermute only.
A program may use at most 128 MiB of HBM per device.

```python
import math
import jax
import jax.numpy as jnp
from jax import lax

D = 8192
RANK = 512
COLS = 1024
TOKENS = 4096


def level_of(own_key, shape, pieces, least, high):
    def one(position, parts):
        heights = jax.random.uniform(jax.random.fold_in(jax.random.fold_in(own_key, 6), position), (parts,), jnp.float32, least / len(pieces), high / len(pieces))
        return jnp.repeat(jnp.exp(heights), shape[position] // parts).reshape((-1,) + (1,) * (len(shape) - position - 1))

    level = one(*pieces[0])
    for cut in pieces[1:]:
        level = level * one(*cut)
    return level


def gaussian(stream_key, dims, scale, limit, cuts=(), dtype=jnp.bfloat16):
    values = jax.random.normal(stream_key, dims, jnp.float32) * scale
    if len(cuts) > 0:
        values = level_of(stream_key, dims, cuts, -0.22, 0.18) * values
    return jnp.clip(values, min=-limit, max=limit).astype(dtype)


def setup_inputs(seed: int = 0) -> dict:
    arg_keys = jax.random.split(jax.random.key(seed), 7)
    return {
        "activations": gaussian(arg_keys[0], (TOKENS, D), 1.0, 6.0, ((0, 8), (1, 4))),
        "out_grads": gaussian(arg_keys[1], (TOKENS, COLS), 0.011, 0.06591797, ((0, 8),)),
        "projector": gaussian(arg_keys[2], (D, RANK), D ** -0.5, 0.0625, ((0, 4),)),
        "weight": gaussian(arg_keys[3], (D, COLS), 0.00004, 0.00024, ((0, 4),), jnp.float32),
        "first_moment": gaussian(arg_keys[4], (RANK, COLS), 0.1, 0.6, ((0, 8), (1, 4)), jnp.float32),
        "second_moment": jnp.clip(jnp.exp(math.log(0.003) - 2.3025851 * jax.random.uniform(arg_keys[5], (RANK, COLS), jnp.float32) ** level_of(arg_keys[5], (RANK, COLS), ((0, 8), (1, 4)), -0.2, 0.2)), 0.0003, 0.003),
    }


first_decay = 0.9
second_decay = 0.999
first_bias = 1.0 - 0.9 ** 2
second_bias = 1.0 - 0.999 ** 2
epsilon = 1e-08
step_rate = 0.00025

def reference(activations, out_grads, projector, weight, first_moment, second_moment):
    basis = projector.astype(jnp.float32)
    projected = jnp.dot(activations.astype(jnp.float32), basis, precision=lax.Precision.HIGHEST)
    coefficients = jnp.dot(projected.T, out_grads.astype(jnp.float32), precision=lax.Precision.HIGHEST)
    first_new = first_decay * first_moment + (1.0 - first_decay) * coefficients
    second_new = second_decay * second_moment + (1.0 - second_decay) * coefficients * coefficients
    normalized = (first_new / first_bias / (jnp.sqrt(second_new / second_bias) + epsilon)).astype(jnp.bfloat16)
    expanded = jnp.dot(basis, normalized.astype(jnp.float32), precision=lax.Precision.HIGHEST)
    new_weight = weight - step_rate * expanded
    return (new_weight, expanded.astype(jnp.bfloat16), first_new, second_new)
```

```python
import functools

import jax
import jax.numpy as jnp
from jax import lax
from jax.experimental import pallas as pl
from jax.experimental.pallas import tpu as pltpu
from jax.sharding import PartitionSpec as P


first_decay = 0.9
second_decay = 0.999
first_bias = 1.0 - 0.9**2
second_bias = 1.0 - 0.999**2
epsilon = 1e-08
step_rate = 0.00025


def stages(n):
    out, stride = [], 1
    while stride < n:
        left = n // stride
        if stride == 1 and left % 2 == 0:
            f = 2
        elif left % 4 == 0:
            f = 4
        elif left % 2 == 0:
            f = 2
        else:
            f = left
        out.append((stride, f))
        stride *= f
    return out


def other(d, k, f):
    if f & (f - 1) == 0:
        return d ^ k, d ^ k
    return (d + k) % f, (d - k + f) % f


def shift(x, axis, n, stride, f, k):
    pairs = []
    for i in range(n):
        d = (i // stride) % f
        pairs.append((i, i + (other(d, k, f)[0] - d) * stride))
    return lax.ppermute(x, axis, pairs)


def block(x, i):
    return lax.dynamic_index_in_dim(x, i, axis=1, keepdims=False)


def scatter_stage(kept, sends, axis, n, stride, f):
    for k in range(1, f):
        kept = kept + shift(sends[k - 1], axis, n, stride, f, k).astype(jnp.float32)
    return kept


def digits_of(axis, stride, f):
    d = (lax.axis_index(axis) // stride) % f
    return d, [other(d, k, f)[0] for k in range(1, f)]


def scatter_rows(x, axis, n, stride, f):
    d, others = digits_of(axis, stride, f)
    x = x.reshape(n // (stride * f), f, -1, x.shape[1])
    pick = lambda i: block(x, i).reshape(-1, x.shape[3])
    return scatter_stage(pick(d), [pick(i).astype(jnp.bfloat16) for i in others], axis, n, stride, f)


def scatter_columns(x, axis, n):
    d, others = digits_of(axis, 1, n)
    width = x.shape[1] // n
    pick = lambda i: lax.dynamic_slice_in_dim(x, i * width, width, axis=1)
    return scatter_stage(pick(d), [pick(i).astype(jnp.bfloat16) for i in others], axis, n, 1, n)


def gather(x, axis, n, plan):
    me = lax.axis_index(axis)
    x = x[None]
    for stride, f in reversed(plan):
        d = (me // stride) % f
        got = [shift(x, axis, n, stride, f, k) for k in range(1, f)]
        full = jnp.zeros((x.shape[0], f) + x.shape[1:], x.dtype)
        full = lax.dynamic_update_index_in_dim(full, x, d, 1)
        for k in range(1, f):
            full = lax.dynamic_update_index_in_dim(full, got[k - 1], other(d, k, f)[1], 1)
        x = full.reshape((x.shape[0] * f,) + x.shape[1:])
    return x


def gather_columns(x, axis, n):
    d, _ = digits_of(axis, 1, n)
    width = x.shape[1]
    full = jnp.zeros((x.shape[0], n * width), x.dtype)
    full = lax.dynamic_update_slice_in_dim(full, x, d * width, 1)
    for k in range(1, n):
        got = shift(x, axis, n, 1, n, k)
        full = lax.dynamic_update_slice_in_dim(full, got, other(d, k, n)[1] * width, 1)
    return full


def front_kernel(f, rows, d_ref, a_ref, p_ref, g_ref, *refs):
    keep_ref, send_refs, (total, turned, picked) = refs[0], refs[1:f], refs[f:]
    step = pl.program_id(0)

    @pl.when(step == 0)
    def _():
        total[...] = jnp.zeros_like(total)

    total[...] += jnp.dot(a_ref[...], p_ref[...], preferred_element_type=jnp.float32)

    @pl.when(step == pl.num_programs(0) - 1)
    def _():
        turned[...] = total[...].T.astype(turned.dtype)
        for k in range(f):
            d = d_ref[k]
            for h in range(picked.shape[0] // rows):
                at = pl.multiple_of((h * f + d) * rows, rows)
                picked[pl.ds(h * rows, rows), :] = turned[pl.ds(at, rows), :]
            part = jnp.dot(picked[...], g_ref[...], preferred_element_type=jnp.float32)
            if k == 0:
                keep_ref[...] = part
            else:
                send_refs[k - 1][...] = part.astype(jnp.bfloat16)


def front(activations, out_grads, projector, digits, f, rows):
    tokens, depth = activations.shape
    rank, width = projector.shape[1], out_grads.shape[1]
    steps = 4
    part = rank // f
    kept = jax.ShapeDtypeStruct((part, width), jnp.float32)
    sent = jax.ShapeDtypeStruct((part, width), jnp.bfloat16)
    fixed = lambda i, d: (0, 0)
    return pl.pallas_call(
        functools.partial(front_kernel, f, rows),
        out_shape=[kept] + [sent] * (f - 1),
        grid_spec=pltpu.PrefetchScalarGridSpec(
            num_scalar_prefetch=1,
            grid=(steps,),
            in_specs=[
                pl.BlockSpec((tokens, depth // steps), lambda i, d: (0, i)),
                pl.BlockSpec((depth // steps, rank), lambda i, d: (i, 0)),
                pl.BlockSpec((tokens, width), fixed),
            ],
            out_specs=[pl.BlockSpec((part, width), fixed)] * f,
            scratch_shapes=[
                pltpu.VMEM((tokens, rank), jnp.float32),
                pltpu.VMEM((rank, tokens), jnp.bfloat16),
                pltpu.VMEM((part, tokens), jnp.bfloat16),
            ],
        ),
        compiler_params=pltpu.CompilerParams(vmem_limit_bytes=60 << 20),
        cost_estimate=pl.CostEstimate(
            flops=2 * tokens * rank * (depth + width),
            bytes_accessed=2 * (tokens * depth + depth * rank + tokens * width) + 4 * rank * width,
            transcendentals=0,
        ),
        name="front",
    )(digits, activations, projector, out_grads)


def expand_kernel(p_ref, n_ref, w_ref, new_ref, update_ref):
    expanded = jnp.dot(p_ref[...], n_ref[...], preferred_element_type=jnp.float32)
    new_ref[...] = w_ref[...] - step_rate * expanded
    update_ref[...] = expanded.astype(update_ref.dtype)


def expand(projector, whole, weight):
    depth, rank = projector.shape
    width = weight.shape[1]
    steps = 8
    tile = pl.BlockSpec((depth // steps, width), lambda i: (i, 0))
    return pl.pallas_call(
        expand_kernel,
        grid=(steps,),
        out_shape=[
            jax.ShapeDtypeStruct(weight.shape, jnp.float32),
            jax.ShapeDtypeStruct(weight.shape, jnp.bfloat16),
        ],
        in_specs=[
            pl.BlockSpec((depth // steps, rank), lambda i: (i, 0)),
            pl.BlockSpec((rank, width), lambda i: (0, 0)),
            tile,
        ],
        out_specs=[tile, tile],
        compiler_params=pltpu.CompilerParams(vmem_limit_bytes=60 << 20),
        cost_estimate=pl.CostEstimate(
            flops=2 * depth * rank * width,
            bytes_accessed=10 * depth * width + 2 * rank * (depth + width),
            transcendentals=0,
        ),
        name="expand",
    )(projector, whole, weight)


def local(ndp, nmp, activations, out_grads, projector, weight, first_moment, second_moment):
    rows, columns = first_moment.shape
    first, *rest = stages(ndp)
    d, others = digits_of("dp", *first)
    digits = jnp.stack([d] + others).astype(jnp.int32)
    kept, *sends = front(activations, out_grads, projector, digits, first[1], rows)
    part = scatter_stage(kept, sends, "dp", ndp, *first)
    for stride, f in rest:
        part = scatter_rows(part, "dp", ndp, stride, f)
    coefficients = scatter_columns(part, "mp", nmp)
    first_new = first_decay * first_moment + (1.0 - first_decay) * coefficients
    second_new = second_decay * second_moment + (1.0 - second_decay) * coefficients * coefficients
    normalized = (first_new / first_bias / (jnp.sqrt(second_new / second_bias) + epsilon)).astype(
        jnp.bfloat16
    )
    wide = gather_columns(normalized, "mp", nmp)
    whole = gather(wide, "dp", ndp, stages(ndp)).reshape(ndp * rows, nmp * columns)
    new_weight, update = expand(projector, whole, weight)
    return (new_weight, update, first_new, second_new)


def solution(mesh):
    ndp, nmp = mesh.shape["dp"], mesh.shape["mp"]
    in_specs = (
        P("dp", "mp"),
        P("dp", None),
        P("mp", None),
        P("mp", None),
        P("dp", "mp"),
        P("dp", "mp"),
    )
    out_specs = (P("mp", None), P("mp", None), P("dp", "mp"), P("dp", "mp"))

    def step(*args):
        return local(ndp, nmp, *args)

    return jax.shard_map(step, mesh=mesh, in_specs=in_specs, out_specs=out_specs, check_vma=False)
```

```python
import functools
import math

import jax
import jax.numpy as jnp
from jax import lax
from jax.experimental import pallas as pl
from jax.experimental.pallas import tpu as pltpu
from jax.sharding import PartitionSpec as P


first_decay = 0.9
second_decay = 0.999
first_bias = 1.0 - 0.9**2
second_bias = 1.0 - 0.999**2
epsilon = 1e-08
step_rate = 0.00025


def stages(n):
    out, stride = [], 1
    while stride < n:
        left = n // stride
        if stride == 1 and left % 2 == 0:
            f = 2
        elif left % 4 == 0:
            f = 4
        elif left % 2 == 0:
            f = 2
        else:
            f = left
        out.append((stride, f))
        stride *= f
    return out


def other(d, k, f):
    if f & (f - 1) == 0:
        return d ^ k, d ^ k
    return (d + k) % f, (d - k + f) % f


def shift(x, axis, n, stride, f, k):
    pairs = []
    for i in range(n):
        d = (i // stride) % f
        pairs.append((i, i + (other(d, k, f)[0] - d) * stride))
    return lax.ppermute(x, axis, pairs)


def fits(*shapes):
    size = sum(math.prod(x.shape) * x.dtype.itemsize for x in shapes)
    return pltpu.CompilerParams(vmem_limit_bytes=int(size) + (1 << 20))


def on_chip(kernel, out, *args, name, flops=0):
    vmem = pl.BlockSpec(memory_space=pltpu.VMEM)
    size = sum(math.prod(x.shape) * x.dtype.itemsize for x in [*args, *out])
    return pl.pallas_call(
        kernel,
        out_shape=[pltpu.VMEM(x.shape, x.dtype) for x in out],
        in_specs=[vmem] * len(args),
        out_specs=[vmem] * len(out),
        compiler_params=fits(*args, *out),
        cost_estimate=pl.CostEstimate(flops=flops, bytes_accessed=size, transcendentals=0),
        name=name,
    )(*args)


def exchange(sends, axis, n, stride, f):
    return [shift(x, axis, n, stride, f, k + 1) for k, x in enumerate(sends)]


def digit(axis, stride, f):
    return (lax.axis_index(axis) // stride) % f


def total_of(kept, got, *at):
    x = kept[at]
    for g in got:
        x = x + g[at].astype(jnp.float32)
    return x


def split_rows_kernel(axis, stride, f, rows, count, *refs):
    kept, got, out = refs[0], refs[1:count], refs[count:]
    d = digit(axis, stride, f)
    for k in range(f):
        for h in range(out[k].shape[0] // rows):
            at = pl.multiple_of((h * f + other(d, k, f)[0]) * rows, rows)
            x = total_of(kept, got, pl.ds(at, rows), slice(None))
            out[k][pl.ds(h * rows, rows), :] = x.astype(out[k].dtype)


def split_columns_kernel(axis, f, count, *refs):
    kept, got, out = refs[0], refs[1:count], refs[count:]
    d, width = digit(axis, 1, f), out[0].shape[1]
    for k in range(f):
        at = pl.multiple_of(other(d, k, f)[0] * width, width)
        out[k][...] = total_of(kept, got, slice(None), pl.ds(at, width)).astype(out[k].dtype)


def parts(shape, f):
    wide, narrow = jax.ShapeDtypeStruct(shape, jnp.float32), jax.ShapeDtypeStruct(shape, jnp.bfloat16)
    return [wide] + [narrow] * (f - 1)


def split_rows(kept, got, axis, stride, f, rows):
    kernel = functools.partial(split_rows_kernel, axis, stride, f, rows, 1 + len(got))
    out = parts((kept.shape[0] // f, kept.shape[1]), f)
    kept, *sends = on_chip(kernel, out, kept, *got, name="split_rows")
    return kept, sends


def split_columns(kept, got, axis, f):
    kernel = functools.partial(split_columns_kernel, axis, f, 1 + len(got))
    out = parts((kept.shape[0], kept.shape[1] // f), f)
    kept, *sends = on_chip(kernel, out, kept, *got, name="split_columns")
    return kept, sends


def moments(count, refs):
    c = total_of(refs[0], refs[1:count], slice(None), slice(None))
    first_ref, second_ref = refs[count], refs[count + 1]
    first_new = first_decay * first_ref[...] + (1.0 - first_decay) * c
    second_new = second_decay * second_ref[...] + (1.0 - second_decay) * c * c
    return first_new, second_new


def normalize_kernel(count, *refs):
    first_new, second_new = moments(count, refs)
    x = first_new / first_bias / (jnp.sqrt(second_new / second_bias) + epsilon)
    refs[-1][...] = x.astype(refs[-1].dtype)


def moments_kernel(count, *refs):
    refs[-2][...], refs[-1][...] = moments(count, refs)


def normalize(kept, got, first_moment, second_moment):
    kernel = functools.partial(normalize_kernel, 1 + len(got))
    out = [jax.ShapeDtypeStruct(kept.shape, jnp.bfloat16)]
    return on_chip(kernel, out, kept, *got, first_moment, second_moment, name="normalize")[0]


def new_moments(kept, got, first_moment, second_moment):
    args = [kept, *got, first_moment, second_moment]
    out = [jax.ShapeDtypeStruct(kept.shape, jnp.float32)] * 2
    return pl.pallas_call(
        functools.partial(moments_kernel, 1 + len(got)),
        out_shape=out,
        compiler_params=fits(*args, *out),
        cost_estimate=pl.CostEstimate(flops=1 << 28, bytes_accessed=16 * kept.size, transcendentals=0),
        name="new_moments",
    )(*args)


def join_columns_kernel(axis, f, *refs):
    out, d, width = refs[-1], digit(axis, 1, f), refs[0].shape[1]
    for k in range(f):
        at = pl.multiple_of(other(d, k, f)[1] * width, width)
        out[:, pl.ds(at, width)] = refs[k][...]


def join_columns(x, got, axis, f):
    out = [jax.ShapeDtypeStruct((x.shape[0], x.shape[1] * f), x.dtype)]
    kernel = functools.partial(join_columns_kernel, axis, f)
    return on_chip(kernel, out, x, *got, name="join_columns")[0]


def join_rows_kernel(axis, stride, f, rows, *refs):
    out, d = refs[-1], digit(axis, stride, f)
    for k in range(f):
        for h in range(refs[k].shape[0] // rows):
            at = pl.multiple_of((h * f + other(d, k, f)[1]) * rows, rows)
            out[pl.ds(at, rows), :] = refs[k][pl.ds(h * rows, rows), :]


def join_rows(x, got, axis, stride, f, rows):
    out = [jax.ShapeDtypeStruct((x.shape[0] * f, x.shape[1]), x.dtype)]
    kernel = functools.partial(join_rows_kernel, axis, stride, f, rows)
    return on_chip(kernel, out, x, *got, name="join_rows")[0]


def in_vmem(shape, dtype):
    return pltpu.VMEM(shape, dtype)


def front_kernel(ndp, f, rows, a_hbm, p_hbm, g_hbm, *refs):
    keep_ref, send_refs, (p_ref, a_ref, g_ref, total, turned, picked, sems) = refs[0], refs[1:f], refs[f:]
    depth = a_ref.shape[1]
    steps = sems.shape[1]
    tile = depth // steps
    copies = []
    for i in range(steps):
        cut = pl.ds(i * tile, tile)
        copies.append(
            (
                pltpu.make_async_copy(a_hbm.at[:, cut], a_ref.at[:, cut], sems.at[0, i]),
                pltpu.make_async_copy(p_hbm.at[cut, :], p_ref.at[cut, :], sems.at[1, i]),
            )
        )
    late = pltpu.make_async_copy(g_hbm, g_ref, sems.at[2, 0])
    for pair in copies:
        for copy in pair:
            copy.start()
    late.start()
    for i, pair in enumerate(copies):
        for copy in pair:
            copy.wait()
        cut = pl.ds(i * tile, tile)
        part = jnp.dot(a_ref[:, cut], p_ref[cut, :], preferred_element_type=jnp.float32)
        total[...] = part if i == 0 else total[...] + part
    turned[...] = total[...].astype(turned.dtype).T
    late.wait()
    mine = digit("dp", 1, f)
    for k in [*range(1, f), 0]:
        d = other(mine, k, f)[0]
        for h in range(picked.shape[0] // rows):
            at = pl.multiple_of((h * f + d) * rows, rows)
            picked[pl.ds(h * rows, rows), :] = turned[pl.ds(at, rows), :]
        part = jnp.dot(picked[...], g_ref[...], preferred_element_type=jnp.float32)
        if k == 0:
            keep_ref[...] = part
        else:
            send_refs[k - 1][...] = part.astype(jnp.bfloat16)


def front(activations, out_grads, projector, ndp, f, rows):
    tokens, depth = activations.shape
    rank, width = projector.shape[1], out_grads.shape[1]
    part = rank // f
    hbm = pl.BlockSpec(memory_space=pltpu.HBM)
    vmem = pl.BlockSpec(memory_space=pltpu.VMEM)
    *out, copy = pl.pallas_call(
        functools.partial(front_kernel, ndp, f, rows),
        out_shape=[in_vmem((part, width), jnp.float32)]
        + [in_vmem((part, width), jnp.bfloat16)] * (f - 1)
        + [in_vmem(projector.shape, projector.dtype)],
        in_specs=[hbm] * 3,
        out_specs=[vmem] * (f + 1),
        scratch_shapes=[
            pltpu.VMEM((tokens, depth), jnp.bfloat16),
            pltpu.VMEM((tokens, width), jnp.bfloat16),
            pltpu.VMEM((tokens, rank), jnp.float32),
            pltpu.VMEM((rank, tokens), jnp.bfloat16),
            pltpu.VMEM((part, tokens), jnp.bfloat16),
            pltpu.SemaphoreType.DMA((3, 4)),
        ],
        compiler_params=pltpu.CompilerParams(vmem_limit_bytes=16 << 20),
        cost_estimate=pl.CostEstimate(
            flops=2 * tokens * rank * (depth + width),
            bytes_accessed=2 * (tokens * depth + depth * rank + tokens * width),
            transcendentals=0,
        ),
        name="front",
    )(
        pltpu.with_memory_space_constraint(activations, pltpu.HBM),
        pltpu.with_memory_space_constraint(projector, pltpu.HBM),
        pltpu.with_memory_space_constraint(out_grads, pltpu.HBM),
    )
    return out, copy


def load_kernel(w_hbm, after_ref, w_ref, sem):
    copy = pltpu.make_async_copy(w_hbm, w_ref, sem)
    copy.start()
    copy.wait()


def load(weight, after):
    return pl.pallas_call(
        load_kernel,
        out_shape=in_vmem(weight.shape, weight.dtype),
        in_specs=[pl.BlockSpec(memory_space=pltpu.HBM), pl.BlockSpec(memory_space=pl.ANY)],
        out_specs=pl.BlockSpec(memory_space=pltpu.VMEM),
        scratch_shapes=[pltpu.SemaphoreType.DMA],
        compiler_params=pltpu.CompilerParams(vmem_limit_bytes=1 << 20),
        cost_estimate=pl.CostEstimate(
            flops=600 * weight.size, bytes_accessed=4 * weight.size, transcendentals=0
        ),
        name="load",
    )(pltpu.with_memory_space_constraint(weight, pltpu.HBM), after)


def expand_kernel(f, rows, p_ref, w_ref, *refs):
    pieces, (new_ref, update_ref, whole) = refs[:f], refs[f:]

    @pl.when(pl.program_id(0) == 0)
    def _():
        join_rows_kernel("dp", 1, f, rows, *pieces, whole)

    tile = new_ref.shape[0]
    cut = pl.ds(pl.multiple_of(pl.program_id(0) * tile, tile), tile)
    expanded = jnp.dot(p_ref[cut, :], whole[...], preferred_element_type=jnp.float32)
    new_ref[...] = w_ref[cut, :] - step_rate * expanded
    update_ref[...] = expanded.astype(update_ref.dtype)


def expand(projector, weight, pieces, rows):
    depth, rank = projector.shape
    width = weight.shape[1]
    steps, f = 8, len(pieces)
    tile = pl.BlockSpec((depth // steps, width), lambda i: (i, 0))
    return pl.pallas_call(
        functools.partial(expand_kernel, f, rows),
        grid=(steps,),
        out_shape=[
            jax.ShapeDtypeStruct(weight.shape, jnp.float32),
            jax.ShapeDtypeStruct(weight.shape, jnp.bfloat16),
        ],
        in_specs=[pl.BlockSpec(memory_space=pltpu.VMEM)] * (2 + f),
        out_specs=[tile, tile],
        scratch_shapes=[pltpu.VMEM((rank, width), jnp.bfloat16)],
        compiler_params=pltpu.CompilerParams(vmem_limit_bytes=12 << 20),
        cost_estimate=pl.CostEstimate(
            flops=2 * depth * rank * width,
            bytes_accessed=10 * depth * width + 2 * rank * (depth + width),
            transcendentals=0,
        ),
        name="expand",
    )(projector, weight, *pieces)


def local(ndp, nmp, activations, out_grads, projector, weight, first_moment, second_moment):
    rows, columns = first_moment.shape
    first, *rest = stages(ndp)
    (kept, *sends), projector = front(activations, out_grads, projector, ndp, first[1], rows)
    got = exchange(sends, "dp", ndp, *first)
    for i, (stride, f) in enumerate(rest):
        kept, sends = split_rows(kept, got, "dp", stride, f, rows)
        if i == 0:
            weight = load(weight, kept)
        got = exchange(sends, "dp", ndp, stride, f)
        if i == 0:
            got, weight = lax.optimization_barrier((got, weight))
    kept, sends = split_columns(kept, got, "mp", nmp)
    got = exchange(sends, "mp", nmp, 1, nmp)
    first_new, second_new = new_moments(kept, got, first_moment, second_moment)
    x = normalize(kept, got, first_moment, second_moment)
    x = join_columns(x, exchange([x] * (nmp - 1), "mp", nmp, 1, nmp), "mp", nmp)
    for stride, f in reversed(rest):
        x = join_rows(x, exchange([x] * (f - 1), "dp", ndp, stride, f), "dp", stride, f, rows)
    pieces = [x] + exchange([x] * (first[1] - 1), "dp", ndp, *first)
    new_weight, update = expand(projector, weight, pieces, rows)
    return (new_weight, update, first_new, second_new)


def solution(mesh):
    ndp, nmp = mesh.shape["dp"], mesh.shape["mp"]
    in_specs = (
        P("dp", "mp"),
        P("dp", None),
        P("mp", None),
        P("mp", None),
        P("dp", "mp"),
        P("dp", "mp"),
    )
    out_specs = (P("mp", None), P("mp", None), P("dp", "mp"), P("dp", "mp"))

    def step(*args):
        return local(ndp, nmp, *args)

    return jax.shard_map(step, mesh=mesh, in_specs=in_specs, out_specs=out_specs, check_vma=False)
```

```python
import functools
import math

import jax
import jax.numpy as jnp
from jax import lax
from jax.experimental import pallas as pl
from jax.experimental.pallas import tpu as pltpu
from jax.sharding import PartitionSpec as P


first_decay = 0.9
second_decay = 0.999
first_bias = 1.0 - 0.9**2
second_bias = 1.0 - 0.999**2
epsilon = 1e-08
EARLY = 0
step_rate = 0.00025


def stages(n):
    out, stride = [], 1
    while stride < n:
        left = n // stride
        if stride == 1 and left % 2 == 0:
            f = 2
        elif left % 4 == 0:
            f = 4
        elif left % 2 == 0:
            f = 2
        else:
            f = left
        out.append((stride, f))
        stride *= f
    return out


def other(d, k, f):
    if f & (f - 1) == 0:
        return d ^ k, d ^ k
    return (d + k) % f, (d - k + f) % f


def shift(x, axis, n, stride, f, k):
    pairs = []
    for i in range(n):
        d = (i // stride) % f
        pairs.append((i, i + (other(d, k, f)[0] - d) * stride))
    return lax.ppermute(x, axis, pairs)


def fits(*shapes):
    size = sum(math.prod(x.shape) * x.dtype.itemsize for x in shapes)
    return pltpu.CompilerParams(vmem_limit_bytes=int(size) + (1 << 20))


def on_chip(kernel, out, *args, name, flops=0):
    vmem = pl.BlockSpec(memory_space=pltpu.VMEM)
    size = sum(math.prod(x.shape) * x.dtype.itemsize for x in [*args, *out])
    return pl.pallas_call(
        kernel,
        out_shape=[pltpu.VMEM(x.shape, x.dtype) for x in out],
        in_specs=[vmem] * len(args),
        out_specs=[vmem] * len(out),
        compiler_params=fits(*args, *out),
        cost_estimate=pl.CostEstimate(flops=flops, bytes_accessed=size, transcendentals=0),
        name=name,
    )(*args)


def exchange(sends, axis, n, stride, f):
    return [shift(x, axis, n, stride, f, k + 1) for k, x in enumerate(sends)]


def digit(axis, stride, f):
    return (lax.axis_index(axis) // stride) % f


def total_of(kept, got, *at):
    x = kept[at]
    for g in got:
        x = x + g[at].astype(jnp.float32)
    return x


def split_rows_kernel(axis, stride, f, rows, count, *refs):
    kept, got, out = refs[0], refs[1:count], refs[count:]
    d = digit(axis, stride, f)
    for k in range(f):
        for h in range(out[k].shape[0] // rows):
            at = pl.multiple_of((h * f + other(d, k, f)[0]) * rows, rows)
            x = total_of(kept, got, pl.ds(at, rows), slice(None))
            out[k][pl.ds(h * rows, rows), :] = x.astype(out[k].dtype)


def split_columns_kernel(axis, f, count, *refs):
    kept, got, out = refs[0], refs[1:count], refs[count:]
    d, width = digit(axis, 1, f), out[0].shape[1]
    for k in range(f):
        at = pl.multiple_of(other(d, k, f)[0] * width, width)
        out[k][...] = total_of(kept, got, slice(None), pl.ds(at, width)).astype(out[k].dtype)


def parts(shape, f):
    wide, narrow = jax.ShapeDtypeStruct(shape, jnp.float32), jax.ShapeDtypeStruct(shape, jnp.bfloat16)
    return [wide] + [narrow] * (f - 1)


def split_rows(kept, got, axis, stride, f, rows):
    kernel = functools.partial(split_rows_kernel, axis, stride, f, rows, 1 + len(got))
    out = parts((kept.shape[0] // f, kept.shape[1]), f)
    kept, *sends = on_chip(kernel, out, kept, *got, name="split_rows")
    return kept, sends


def split_columns(kept, got, axis, f):
    kernel = functools.partial(split_columns_kernel, axis, f, 1 + len(got))
    out = parts((kept.shape[0], kept.shape[1] // f), f)
    kept, *sends = on_chip(kernel, out, kept, *got, name="split_columns")
    return kept, sends


def turns(nmp, stride, first):
    f = nmp
    along_dp = lax.axis_index("dp") % stride == first
    q, z = digit("dp", stride, f), digit("mp", 1, f)
    return along_dp, lax.select(along_dp, q, z), lax.select(along_dp, z, q)


def cross(sends, ndp, nmp, stride, early):
    got = []
    for k, x in enumerate(sends, 1):
        pairs = []
        for dp in range(ndp):
            for mp in range(nmp):
                q = (dp // stride) % nmp
                if dp % stride == early:
                    to = (dp + (other(q, k, nmp)[0] - q) * stride) * nmp + mp
                else:
                    to = dp * nmp + other(mp, k, nmp)[0]
                pairs.append((dp * nmp + mp, to))
        got.append(lax.ppermute(x, ("dp", "mp"), pairs))
    return got


def cross_split_kernel(f, stride, first, rows, width, count, *refs):
    kept, got, out = refs[0], refs[1:count], refs[count:]
    along_dp, mine, _ = turns(f, stride, first)
    for k in range(f):
        d = other(mine, k, f)[0]
        for o in range(f):
            h, j = lax.select(along_dp, d, o), lax.select(along_dp, o, d)
            at = pl.ds(pl.multiple_of(h * rows, rows), rows), pl.ds(pl.multiple_of(j * width, width), width)
            out[k][pl.ds(o * rows, rows), :] = total_of(kept, got, *at).astype(out[k].dtype)


def cross_split(kept, got, f, stride, first, rows, width):
    kernel = functools.partial(cross_split_kernel, f, stride, first, rows, width, 1 + len(got))
    kept, *sends = on_chip(kernel, parts((f * rows, width), f), kept, *got, name="cross_split")
    return kept, sends


def second_split_kernel(f, stride, first, rows, count, *refs):
    kept, got, out = refs[0], refs[1:count], refs[count:]
    mine = turns(f, stride, first)[2]
    for k in range(f):
        at = pl.multiple_of(other(mine, k, f)[0] * rows, rows)
        out[k][...] = total_of(kept, got, pl.ds(at, rows), slice(None)).astype(out[k].dtype)


def second_split(kept, got, f, stride, first, rows):
    kernel = functools.partial(second_split_kernel, f, stride, first, rows, 1 + len(got))
    kept, *sends = on_chip(kernel, parts((rows, kept.shape[1]), f), kept, *got, name="second_split")
    return kept, sends


def first_join_kernel(f, stride, first, rows, *refs):
    out, mine = refs[-1], turns(f, stride, first)[2]
    for k in range(f):
        at = pl.multiple_of(other(mine, k, f)[1] * rows, rows)
        out[pl.ds(at, rows), :] = refs[k][...]


def first_join(x, got, f, stride, first):
    rows, width = x.shape
    kernel = functools.partial(first_join_kernel, f, stride, first, rows)
    out = [jax.ShapeDtypeStruct((f * rows, width), x.dtype)]
    return on_chip(kernel, out, x, *got, name="first_join")[0]


def cross_join_kernel(f, stride, first, rows, *refs):
    out, width = refs[-1], refs[0].shape[1]
    along_dp, mine, _ = turns(f, stride, first)
    for k in range(f):
        d = other(mine, k, f)[1]
        for o in range(f):
            h, j = lax.select(along_dp, d, o), lax.select(along_dp, o, d)
            at = pl.ds(pl.multiple_of(h * rows, rows), rows), pl.ds(pl.multiple_of(j * width, width), width)
            out[at] = refs[k][pl.ds(o * rows, rows), :]


def cross_join(x, got, f, stride, first, rows):
    kernel = functools.partial(cross_join_kernel, f, stride, first, rows)
    out = [jax.ShapeDtypeStruct((f * rows, f * x.shape[1]), x.dtype)]
    return on_chip(kernel, out, x, *got, name="cross_join")[0]


def moments(count, refs):
    c = total_of(refs[0], refs[1:count], slice(None), slice(None))
    first_ref, second_ref = refs[count], refs[count + 1]
    first_new = first_decay * first_ref[...] + (1.0 - first_decay) * c
    second_new = second_decay * second_ref[...] + (1.0 - second_decay) * c * c
    return first_new, second_new


def normalize_kernel(count, *refs):
    first_new, second_new = moments(count, refs)
    x = first_new / first_bias / (jnp.sqrt(second_new / second_bias) + epsilon)
    refs[-1][...] = x.astype(refs[-1].dtype)


def moments_kernel(count, *refs):
    refs[-2][...], refs[-1][...] = moments(count, refs)


def normalize(kept, got, first_moment, second_moment):
    kernel = functools.partial(normalize_kernel, 1 + len(got))
    out = [jax.ShapeDtypeStruct(kept.shape, jnp.bfloat16)]
    return on_chip(kernel, out, kept, *got, first_moment, second_moment, name="normalize")[0]


def new_moments(kept, got, first_moment, second_moment):
    args = [kept, *got, first_moment, second_moment]
    out = [jax.ShapeDtypeStruct(kept.shape, jnp.float32)] * 2
    return pl.pallas_call(
        functools.partial(moments_kernel, 1 + len(got)),
        out_shape=out,
        compiler_params=fits(*args, *out),
        cost_estimate=pl.CostEstimate(flops=1 << 28, bytes_accessed=16 * kept.size, transcendentals=0),
        name="new_moments",
    )(*args)


def join_columns_kernel(axis, f, *refs):
    out, d, width = refs[-1], digit(axis, 1, f), refs[0].shape[1]
    for k in range(f):
        at = pl.multiple_of(other(d, k, f)[1] * width, width)
        out[:, pl.ds(at, width)] = refs[k][...]


def join_columns(x, got, axis, f):
    out = [jax.ShapeDtypeStruct((x.shape[0], x.shape[1] * f), x.dtype)]
    kernel = functools.partial(join_columns_kernel, axis, f)
    return on_chip(kernel, out, x, *got, name="join_columns")[0]


def join_rows_kernel(axis, stride, f, rows, *refs):
    out, d = refs[-1], digit(axis, stride, f)
    for k in range(f):
        for h in range(refs[k].shape[0] // rows):
            at = pl.multiple_of((h * f + other(d, k, f)[1]) * rows, rows)
            out[pl.ds(at, rows), :] = refs[k][pl.ds(h * rows, rows), :]


def join_rows(x, got, axis, stride, f, rows):
    out = [jax.ShapeDtypeStruct((x.shape[0] * f, x.shape[1]), x.dtype)]
    kernel = functools.partial(join_rows_kernel, axis, stride, f, rows)
    return on_chip(kernel, out, x, *got, name="join_rows")[0]


def in_vmem(shape, dtype):
    return pltpu.VMEM(shape, dtype)


def front_kernel(ndp, f, rows, a_hbm, p_hbm, g_hbm, *refs):
    send_refs, (p_ref, turned, g_ref, a_ref, total, picked, sems) = refs[: f - 1], refs[f - 1 :]
    depth = a_ref.shape[1]
    steps = sems.shape[1]
    tile = depth // steps
    copies = []
    for i in range(steps):
        cut = pl.ds(i * tile, tile)
        copies.append(
            (
                pltpu.make_async_copy(a_hbm.at[:, cut], a_ref.at[:, cut], sems.at[0, i]),
                pltpu.make_async_copy(p_hbm.at[cut, :], p_ref.at[cut, :], sems.at[1, i]),
            )
        )
    late = pltpu.make_async_copy(g_hbm, g_ref, sems.at[2, 0])
    for pair in copies:
        for copy in pair:
            copy.start()
    late.start()
    for i, pair in enumerate(copies):
        for copy in pair:
            copy.wait()
        cut = pl.ds(i * tile, tile)
        part = jnp.dot(a_ref[:, cut], p_ref[cut, :], preferred_element_type=jnp.float32)
        total[...] = part if i == 0 else total[...] + part
    turned[...] = total[...].astype(turned.dtype).T
    late.wait()
    half_kernel(f, rows, range(1, f), turned, g_ref, picked, send_refs)


def half_kernel(f, rows, which, turned, g_ref, picked, out):
    mine = digit("dp", 1, f)
    for k, ref in zip(which, out):
        d = other(mine, k, f)[0]
        for h in range(picked.shape[0] // rows):
            at = pl.multiple_of((h * f + d) * rows, rows)
            picked[pl.ds(h * rows, rows), :] = turned[pl.ds(at, rows), :]
        part = jnp.dot(picked[...], g_ref[...], preferred_element_type=jnp.float32)
        ref[...] = part.astype(ref.dtype)


def keep_kernel(f, rows, turned, g_ref, keep_ref, picked):
    half_kernel(f, rows, [0], turned, g_ref, picked, [keep_ref])


def keep(turned, out_grads, f, rows):
    rank, tokens = turned.shape
    width = out_grads.shape[1]
    out = jax.ShapeDtypeStruct((rank // f, width), jnp.float32)
    return pl.pallas_call(
        functools.partial(keep_kernel, f, rows),
        out_shape=pltpu.VMEM(out.shape, out.dtype),
        in_specs=[pl.BlockSpec(memory_space=pltpu.VMEM)] * 2,
        out_specs=pl.BlockSpec(memory_space=pltpu.VMEM),
        scratch_shapes=[pltpu.VMEM((rank // f, tokens), jnp.bfloat16)],
        compiler_params=fits(turned, out_grads, out),
        cost_estimate=pl.CostEstimate(
            flops=2 * tokens * rank * width // f, bytes_accessed=4 * out.size, transcendentals=0
        ),
        name="keep",
    )(turned, out_grads)


def front(activations, out_grads, projector, ndp, f, rows):
    tokens, depth = activations.shape
    rank, width = projector.shape[1], out_grads.shape[1]
    part = rank // f
    hbm = pl.BlockSpec(memory_space=pltpu.HBM)
    vmem = pl.BlockSpec(memory_space=pltpu.VMEM)
    *sends, copy, turned, grads = pl.pallas_call(
        functools.partial(front_kernel, ndp, f, rows),
        out_shape=[in_vmem((part, width), jnp.bfloat16)] * (f - 1)
        + [
            in_vmem(projector.shape, projector.dtype),
            in_vmem((rank, tokens), jnp.bfloat16),
            in_vmem(out_grads.shape, out_grads.dtype),
        ],
        in_specs=[hbm] * 3,
        out_specs=[vmem] * (f + 2),
        scratch_shapes=[
            pltpu.VMEM((tokens, depth), jnp.bfloat16),
            pltpu.VMEM((tokens, rank), jnp.float32),
            pltpu.VMEM((part, tokens), jnp.bfloat16),
            pltpu.SemaphoreType.DMA((3, 4)),
        ],
        compiler_params=pltpu.CompilerParams(vmem_limit_bytes=16 << 20),
        cost_estimate=pl.CostEstimate(
            flops=2 * tokens * rank * (depth + width),
            bytes_accessed=2 * (tokens * depth + depth * rank + tokens * width),
            transcendentals=0,
        ),
        name="front",
    )(
        pltpu.with_memory_space_constraint(activations, pltpu.HBM),
        pltpu.with_memory_space_constraint(projector, pltpu.HBM),
        pltpu.with_memory_space_constraint(out_grads, pltpu.HBM),
    )
    return sends, copy, turned, grads


def load_kernel(w_hbm, after_ref, w_ref, sem):
    copy = pltpu.make_async_copy(w_hbm, w_ref, sem)
    copy.start()
    copy.wait()


def load(weight, after):
    return pl.pallas_call(
        load_kernel,
        out_shape=in_vmem(weight.shape, weight.dtype),
        in_specs=[pl.BlockSpec(memory_space=pltpu.HBM), pl.BlockSpec(memory_space=pl.ANY)],
        out_specs=pl.BlockSpec(memory_space=pltpu.VMEM),
        scratch_shapes=[pltpu.SemaphoreType.DMA],
        compiler_params=pltpu.CompilerParams(vmem_limit_bytes=1 << 20),
        cost_estimate=pl.CostEstimate(
            flops=600 * weight.size, bytes_accessed=4 * weight.size, transcendentals=0
        ),
        name="load",
    )(pltpu.with_memory_space_constraint(weight, pltpu.HBM), after)


def expand_kernel(f, rows, p_ref, w_ref, *refs):
    pieces, (new_hbm, update_hbm, whole, new_ref, update_ref, sems) = refs[:f], refs[f:]
    join_rows_kernel("dp", 1, f, rows, *pieces, whole)
    steps = sems.shape[1]
    tile = w_ref.shape[0] // steps

    def copies(i):
        cut = pl.ds(pl.multiple_of(i * tile, tile), tile)
        return (
            pltpu.make_async_copy(new_ref.at[cut, :], new_hbm.at[cut, :], sems.at[0, i]),
            pltpu.make_async_copy(update_ref.at[cut, :], update_hbm.at[cut, :], sems.at[1, i]),
        )

    @pl.loop(0, steps)
    def _(i):
        cut = pl.ds(pl.multiple_of(i * tile, tile), tile)
        expanded = jnp.dot(p_ref[cut, :], whole[...], preferred_element_type=jnp.float32)
        new_ref[cut, :] = w_ref[cut, :] - step_rate * expanded
        update_ref[cut, :] = expanded.astype(update_ref.dtype)
        for copy in copies(i):
            copy.start()

    @pl.loop(0, steps)
    def _(i):
        for copy in copies(i):
            copy.wait()


def expand(projector, weight, pieces, rows):
    depth, rank = projector.shape
    width = weight.shape[1]
    steps, f = 8, len(pieces)
    return pl.pallas_call(
        functools.partial(expand_kernel, f, rows),
        out_shape=[
            jax.ShapeDtypeStruct(weight.shape, jnp.float32),
            jax.ShapeDtypeStruct(weight.shape, jnp.bfloat16),
        ],
        in_specs=[pl.BlockSpec(memory_space=pltpu.VMEM)] * (2 + f),
        out_specs=[pl.BlockSpec(memory_space=pltpu.HBM)] * 2,
        scratch_shapes=[
            pltpu.VMEM((rank, width), jnp.bfloat16),
            pltpu.VMEM(weight.shape, jnp.float32),
            pltpu.VMEM(weight.shape, jnp.bfloat16),
            pltpu.SemaphoreType.DMA((2, steps)),
        ],
        compiler_params=pltpu.CompilerParams(vmem_limit_bytes=20 << 20),
        cost_estimate=pl.CostEstimate(
            flops=2 * depth * rank * width,
            bytes_accessed=10 * depth * width + 2 * rank * (depth + width),
            transcendentals=0,
        ),
        name="expand",
    )(projector, weight, *pieces)


def local(ndp, nmp, activations, out_grads, projector, weight, first_moment, second_moment):
    rows, columns = first_moment.shape
    first, *rest = stages(ndp)
    pair = first[1]
    sends, projector, turned, grads = front(activations, out_grads, projector, ndp, pair, rows)
    got = exchange(sends, "dp", ndp, *first)
    kept = keep(turned, grads, pair, rows)
    crossed = pair == 2 and rest == [(pair, nmp)]
    if crossed:
        early, late = EARLY, 1 - EARLY
        kept, sends = cross_split(kept, got, nmp, pair, early, rows, columns)
        weight = load(weight, kept)
        got = cross(sends, ndp, nmp, pair, early)
        got, weight = lax.optimization_barrier((got, weight))
        kept, sends = second_split(kept, got, nmp, pair, early, rows)
        got = cross(sends, ndp, nmp, pair, late)
    else:
        for i, (stride, f) in enumerate(rest):
            kept, sends = split_rows(kept, got, "dp", stride, f, rows)
            if i == 0:
                weight = load(weight, kept)
            got = exchange(sends, "dp", ndp, stride, f)
            if i == 0:
                got, weight = lax.optimization_barrier((got, weight))
        kept, sends = split_columns(kept, got, "mp", nmp)
        got = exchange(sends, "mp", nmp, 1, nmp)
    first_new, second_new = new_moments(kept, got, first_moment, second_moment)
    x = normalize(kept, got, first_moment, second_moment)
    if crossed:
        x = first_join(x, cross([x] * (nmp - 1), ndp, nmp, pair, late), nmp, pair, early)
        x = cross_join(x, cross([x] * (nmp - 1), ndp, nmp, pair, early), nmp, pair, early, rows)
    else:
        x = join_columns(x, exchange([x] * (nmp - 1), "mp", nmp, 1, nmp), "mp", nmp)
        for stride, f in reversed(rest):
            x = join_rows(x, exchange([x] * (f - 1), "dp", ndp, stride, f), "dp", stride, f, rows)
    pieces = [x] + exchange([x] * (pair - 1), "dp", ndp, *first)
    new_weight, update = expand(projector, weight, pieces, rows)
    return (new_weight, update, first_new, second_new)


def solution(mesh):
    ndp, nmp = mesh.shape["dp"], mesh.shape["mp"]
    in_specs = (
        P("dp", "mp"),
        P("dp", None),
        P("mp", None),
        P("mp", None),
        P("dp", "mp"),
        P("dp", "mp"),
    )
    out_specs = (P("mp", None), P("mp", None), P("dp", "mp"), P("dp", "mp"))

    def step(*args):
        return local(ndp, nmp, *args)

    return jax.shard_map(step, mesh=mesh, in_specs=in_specs, out_specs=out_specs, check_vma=False)
```

```python
import functools
import math

import jax
import jax.numpy as jnp
from jax import lax
from jax.experimental import pallas as pl
from jax.experimental.pallas import tpu as pltpu
from jax.sharding import PartitionSpec as P


first_decay = 0.9
second_decay = 0.999
first_bias = 1.0 - 0.9**2
second_bias = 1.0 - 0.999**2
epsilon = 1e-08
EARLY = 0
SUMS = (((3, 1, 2), (1, 2, 3)), ((1, 2, 3), (3, 2, 1)))
GATHERS = (((1, 2, 3), (1, 2, 3)), ((1, 2, 3), (1, 2, 3)))
step_rate = 0.00025


def stages(n):
    out, stride = [], 1
    while stride < n:
        left = n // stride
        if stride == 1 and left % 2 == 0:
            f = 2
        elif left % 4 == 0:
            f = 4
        elif left % 2 == 0:
            f = 2
        else:
            f = left
        out.append((stride, f))
        stride *= f
    return out


def other(d, k, f):
    if f & (f - 1) == 0:
        return d ^ k, d ^ k
    return (d + k) % f, (d - k + f) % f


def shift(x, axis, n, stride, f, k):
    pairs = []
    for i in range(n):
        d = (i // stride) % f
        pairs.append((i, i + (other(d, k, f)[0] - d) * stride))
    return lax.ppermute(x, axis, pairs)


def fits(*shapes):
    size = sum(math.prod(x.shape) * x.dtype.itemsize for x in shapes)
    return pltpu.CompilerParams(vmem_limit_bytes=int(size) + (1 << 20))


def on_chip(kernel, out, *args, name, flops=0):
    vmem = pl.BlockSpec(memory_space=pltpu.VMEM)
    size = sum(math.prod(x.shape) * x.dtype.itemsize for x in [*args, *out])
    return pl.pallas_call(
        kernel,
        out_shape=[pltpu.VMEM(x.shape, x.dtype) for x in out],
        in_specs=[vmem] * len(args),
        out_specs=[vmem] * len(out),
        compiler_params=fits(*args, *out),
        cost_estimate=pl.CostEstimate(flops=flops, bytes_accessed=size, transcendentals=0),
        name=name,
    )(*args)


def exchange(sends, axis, n, stride, f):
    return [shift(x, axis, n, stride, f, k + 1) for k, x in enumerate(sends)]


def digit(axis, stride, f):
    return (lax.axis_index(axis) // stride) % f


def total_of(kept, got, *at):
    x = kept[at]
    for g in got:
        x = x + g[at].astype(jnp.float32)
    return x


def split_rows_kernel(axis, stride, f, rows, count, *refs):
    kept, got, out = refs[0], refs[1:count], refs[count:]
    d = digit(axis, stride, f)
    for k in range(f):
        for h in range(out[k].shape[0] // rows):
            at = pl.multiple_of((h * f + other(d, k, f)[0]) * rows, rows)
            x = total_of(kept, got, pl.ds(at, rows), slice(None))
            out[k][pl.ds(h * rows, rows), :] = x.astype(out[k].dtype)


def split_columns_kernel(axis, f, count, *refs):
    kept, got, out = refs[0], refs[1:count], refs[count:]
    d, width = digit(axis, 1, f), out[0].shape[1]
    for k in range(f):
        at = pl.multiple_of(other(d, k, f)[0] * width, width)
        out[k][...] = total_of(kept, got, slice(None), pl.ds(at, width)).astype(out[k].dtype)


def parts(shape, f):
    wide, narrow = jax.ShapeDtypeStruct(shape, jnp.float32), jax.ShapeDtypeStruct(shape, jnp.bfloat16)
    return [wide] + [narrow] * (f - 1)


def split_rows(kept, got, axis, stride, f, rows):
    kernel = functools.partial(split_rows_kernel, axis, stride, f, rows, 1 + len(got))
    out = parts((kept.shape[0] // f, kept.shape[1]), f)
    kept, *sends = on_chip(kernel, out, kept, *got, name="split_rows")
    return kept, sends


def split_columns(kept, got, axis, f):
    kernel = functools.partial(split_columns_kernel, axis, f, 1 + len(got))
    out = parts((kept.shape[0], kept.shape[1] // f), f)
    kept, *sends = on_chip(kernel, out, kept, *got, name="split_columns")
    return kept, sends


def turns(nmp, stride, first):
    f = nmp
    along_dp = lax.axis_index("dp") % stride == first
    q, z = digit("dp", stride, f), digit("mp", 1, f)
    return along_dp, lax.select(along_dp, q, z), lax.select(along_dp, z, q)


def distances(orders, i, f):
    if i == 0 or f != 4:
        return i, i
    return orders[0][i - 1], orders[1][i - 1]


def partner(orders, i, f, along_dp, mine, way):
    p, m = distances(orders, i, f)
    return lax.select(along_dp, other(mine, p, f)[way], other(mine, m, f)[way])


def cross(sends, ndp, nmp, stride, early, orders):
    got = []
    for i, x in enumerate(sends, 1):
        p, m = distances(orders, i, nmp)
        pairs = []
        for dp in range(ndp):
            for mp in range(nmp):
                q = (dp // stride) % nmp
                if dp % stride == early:
                    to = (dp + (other(q, p, nmp)[0] - q) * stride) * nmp + mp
                else:
                    to = dp * nmp + other(mp, m, nmp)[0]
                pairs.append((dp * nmp + mp, to))
        got.append(lax.ppermute(x, ("dp", "mp"), pairs))
    return got


def cross_split_kernel(f, stride, first, rows, width, count, *refs):
    kept, got, out = refs[0], refs[1:count], refs[count:]
    along_dp, mine, _ = turns(f, stride, first)
    for k in range(f):
        d = partner(SUMS[0], k, f, along_dp, mine, 0)
        for o in range(f):
            h, j = lax.select(along_dp, d, o), lax.select(along_dp, o, d)
            at = pl.ds(pl.multiple_of(h * rows, rows), rows), pl.ds(pl.multiple_of(j * width, width), width)
            out[k][pl.ds(o * rows, rows), :] = total_of(kept, got, *at).astype(out[k].dtype)


def cross_split(kept, got, f, stride, first, rows, width):
    kernel = functools.partial(cross_split_kernel, f, stride, first, rows, width, 1 + len(got))
    kept, *sends = on_chip(kernel, parts((f * rows, width), f), kept, *got, name="cross_split")
    return kept, sends


def second_split_kernel(f, stride, first, rows, count, *refs):
    kept, got, out = refs[0], refs[1:count], refs[count:]
    along_dp, _, mine = turns(f, stride, first)
    for k in range(f):
        d = partner(SUMS[1], k, f, jnp.logical_not(along_dp), mine, 0)
        at = pl.multiple_of(d * rows, rows)
        out[k][...] = total_of(kept, got, pl.ds(at, rows), slice(None)).astype(out[k].dtype)


def second_split(kept, got, f, stride, first, rows):
    kernel = functools.partial(second_split_kernel, f, stride, first, rows, 1 + len(got))
    kept, *sends = on_chip(kernel, parts((rows, kept.shape[1]), f), kept, *got, name="second_split")
    return kept, sends


def first_join_kernel(f, stride, first, rows, *refs):
    out, (along_dp, _, mine) = refs[-1], turns(f, stride, first)
    for k in range(f):
        d = partner(GATHERS[0], k, f, jnp.logical_not(along_dp), mine, 1)
        at = pl.multiple_of(d * rows, rows)
        out[pl.ds(at, rows), :] = refs[k][...]


def first_join(x, got, f, stride, first):
    rows, width = x.shape
    kernel = functools.partial(first_join_kernel, f, stride, first, rows)
    out = [jax.ShapeDtypeStruct((f * rows, width), x.dtype)]
    return on_chip(kernel, out, x, *got, name="first_join")[0]


def cross_join_kernel(f, stride, first, rows, *refs):
    out, width = refs[-1], refs[0].shape[1]
    along_dp, mine, _ = turns(f, stride, first)
    for k in range(f):
        d = partner(GATHERS[1], k, f, along_dp, mine, 1)
        for o in range(f):
            h, j = lax.select(along_dp, d, o), lax.select(along_dp, o, d)
            at = pl.ds(pl.multiple_of(h * rows, rows), rows), pl.ds(pl.multiple_of(j * width, width), width)
            out[at] = refs[k][pl.ds(o * rows, rows), :]


def cross_join(x, got, f, stride, first, rows):
    kernel = functools.partial(cross_join_kernel, f, stride, first, rows)
    out = [jax.ShapeDtypeStruct((f * rows, f * x.shape[1]), x.dtype)]
    return on_chip(kernel, out, x, *got, name="cross_join")[0]


def moments(count, refs):
    c = total_of(refs[0], refs[1:count], slice(None), slice(None))
    first_ref, second_ref = refs[count], refs[count + 1]
    first_new = first_decay * first_ref[...] + (1.0 - first_decay) * c
    second_new = second_decay * second_ref[...] + (1.0 - second_decay) * c * c
    return first_new, second_new


def normalize_kernel(count, *refs):
    first_new, second_new = moments(count, refs)
    x = first_new / first_bias / (jnp.sqrt(second_new / second_bias) + epsilon)
    refs[-1][...] = x.astype(refs[-1].dtype)


def moments_kernel(count, *refs):
    refs[-2][...], refs[-1][...] = moments(count, refs)


def normalize(kept, got, first_moment, second_moment):
    kernel = functools.partial(normalize_kernel, 1 + len(got))
    out = [jax.ShapeDtypeStruct(kept.shape, jnp.bfloat16)]
    return on_chip(kernel, out, kept, *got, first_moment, second_moment, name="normalize")[0]


def new_moments(kept, got, first_moment, second_moment):
    args = [kept, *got, first_moment, second_moment]
    out = [jax.ShapeDtypeStruct(kept.shape, jnp.float32)] * 2
    return pl.pallas_call(
        functools.partial(moments_kernel, 1 + len(got)),
        out_shape=out,
        compiler_params=fits(*args, *out),
        cost_estimate=pl.CostEstimate(flops=1 << 28, bytes_accessed=16 * kept.size, transcendentals=0),
        name="new_moments",
    )(*args)


def join_columns_kernel(axis, f, *refs):
    out, d, width = refs[-1], digit(axis, 1, f), refs[0].shape[1]
    for k in range(f):
        at = pl.multiple_of(other(d, k, f)[1] * width, width)
        out[:, pl.ds(at, width)] = refs[k][...]


def join_columns(x, got, axis, f):
    out = [jax.ShapeDtypeStruct((x.shape[0], x.shape[1] * f), x.dtype)]
    kernel = functools.partial(join_columns_kernel, axis, f)
    return on_chip(kernel, out, x, *got, name="join_columns")[0]


def join_rows_kernel(axis, stride, f, rows, *refs):
    out, d = refs[-1], digit(axis, stride, f)
    for k in range(f):
        for h in range(refs[k].shape[0] // rows):
            at = pl.multiple_of((h * f + other(d, k, f)[1]) * rows, rows)
            out[pl.ds(at, rows), :] = refs[k][pl.ds(h * rows, rows), :]


def join_rows(x, got, axis, stride, f, rows):
    out = [jax.ShapeDtypeStruct((x.shape[0] * f, x.shape[1]), x.dtype)]
    kernel = functools.partial(join_rows_kernel, axis, stride, f, rows)
    return on_chip(kernel, out, x, *got, name="join_rows")[0]


def in_vmem(shape, dtype):
    return pltpu.VMEM(shape, dtype)


def front_kernel(ndp, f, rows, a_hbm, p_hbm, g_hbm, *refs):
    send_refs, (p_ref, turned, g_ref, a_ref, total, picked, sems) = refs[: f - 1], refs[f - 1 :]
    depth = a_ref.shape[1]
    steps = sems.shape[1]
    tile = depth // steps
    copies = []
    for i in range(steps):
        cut = pl.ds(i * tile, tile)
        copies.append(
            (
                pltpu.make_async_copy(a_hbm.at[:, cut], a_ref.at[:, cut], sems.at[0, i]),
                pltpu.make_async_copy(p_hbm.at[cut, :], p_ref.at[cut, :], sems.at[1, i]),
            )
        )
    late = pltpu.make_async_copy(g_hbm, g_ref, sems.at[2, 0])
    for pair in copies:
        for copy in pair:
            copy.start()
    late.start()
    for i, pair in enumerate(copies):
        for copy in pair:
            copy.wait()
        cut = pl.ds(i * tile, tile)
        part = jnp.dot(a_ref[:, cut], p_ref[cut, :], preferred_element_type=jnp.float32)
        total[...] = part if i == 0 else total[...] + part
    turned[...] = total[...].astype(turned.dtype).T
    late.wait()
    half_kernel(f, rows, range(1, f), turned, g_ref, picked, send_refs)


def half_kernel(f, rows, which, turned, g_ref, picked, out):
    mine = digit("dp", 1, f)
    for k, ref in zip(which, out):
        d = other(mine, k, f)[0]
        for h in range(picked.shape[0] // rows):
            at = pl.multiple_of((h * f + d) * rows, rows)
            picked[pl.ds(h * rows, rows), :] = turned[pl.ds(at, rows), :]
        part = jnp.dot(picked[...], g_ref[...], preferred_element_type=jnp.float32)
        ref[...] = part.astype(ref.dtype)


def keep_kernel(f, rows, turned, g_ref, keep_ref, picked):
    half_kernel(f, rows, [0], turned, g_ref, picked, [keep_ref])


def keep(turned, out_grads, f, rows):
    rank, tokens = turned.shape
    width = out_grads.shape[1]
    out = jax.ShapeDtypeStruct((rank // f, width), jnp.float32)
    return pl.pallas_call(
        functools.partial(keep_kernel, f, rows),
        out_shape=pltpu.VMEM(out.shape, out.dtype),
        in_specs=[pl.BlockSpec(memory_space=pltpu.VMEM)] * 2,
        out_specs=pl.BlockSpec(memory_space=pltpu.VMEM),
        scratch_shapes=[pltpu.VMEM((rank // f, tokens), jnp.bfloat16)],
        compiler_params=fits(turned, out_grads, out),
        cost_estimate=pl.CostEstimate(
            flops=2 * tokens * rank * width // f, bytes_accessed=4 * out.size, transcendentals=0
        ),
        name="keep",
    )(turned, out_grads)


def front(activations, out_grads, projector, ndp, f, rows):
    tokens, depth = activations.shape
    rank, width = projector.shape[1], out_grads.shape[1]
    part = rank // f
    hbm = pl.BlockSpec(memory_space=pltpu.HBM)
    vmem = pl.BlockSpec(memory_space=pltpu.VMEM)
    *sends, copy, turned, grads = pl.pallas_call(
        functools.partial(front_kernel, ndp, f, rows),
        out_shape=[in_vmem((part, width), jnp.bfloat16)] * (f - 1)
        + [
            in_vmem(projector.shape, projector.dtype),
            in_vmem((rank, tokens), jnp.bfloat16),
            in_vmem(out_grads.shape, out_grads.dtype),
        ],
        in_specs=[hbm] * 3,
        out_specs=[vmem] * (f + 2),
        scratch_shapes=[
            pltpu.VMEM((tokens, depth), jnp.bfloat16),
            pltpu.VMEM((tokens, rank), jnp.float32),
            pltpu.VMEM((part, tokens), jnp.bfloat16),
            pltpu.SemaphoreType.DMA((3, 4)),
        ],
        compiler_params=pltpu.CompilerParams(vmem_limit_bytes=16 << 20),
        cost_estimate=pl.CostEstimate(
            flops=2 * tokens * rank * (depth + width),
            bytes_accessed=2 * (tokens * depth + depth * rank + tokens * width),
            transcendentals=0,
        ),
        name="front",
    )(
        pltpu.with_memory_space_constraint(activations, pltpu.HBM),
        pltpu.with_memory_space_constraint(projector, pltpu.HBM),
        pltpu.with_memory_space_constraint(out_grads, pltpu.HBM),
    )
    return sends, copy, turned, grads


def load_kernel(w_hbm, after_ref, w_ref, sem):
    copy = pltpu.make_async_copy(w_hbm, w_ref, sem)
    copy.start()
    copy.wait()


def load(weight, after):
    return pl.pallas_call(
        load_kernel,
        out_shape=in_vmem(weight.shape, weight.dtype),
        in_specs=[pl.BlockSpec(memory_space=pltpu.HBM), pl.BlockSpec(memory_space=pl.ANY)],
        out_specs=pl.BlockSpec(memory_space=pltpu.VMEM),
        scratch_shapes=[pltpu.SemaphoreType.DMA],
        compiler_params=pltpu.CompilerParams(vmem_limit_bytes=1 << 20),
        cost_estimate=pl.CostEstimate(
            flops=600 * weight.size, bytes_accessed=4 * weight.size, transcendentals=0
        ),
        name="load",
    )(pltpu.with_memory_space_constraint(weight, pltpu.HBM), after)


def expand_kernel(f, rows, p_ref, w_ref, *refs):
    pieces, (new_hbm, update_hbm, whole, new_ref, update_ref, sems) = refs[:f], refs[f:]
    join_rows_kernel("dp", 1, f, rows, *pieces, whole)
    steps = sems.shape[1]
    tile = w_ref.shape[0] // steps

    def copies(i):
        cut = pl.ds(pl.multiple_of(i * tile, tile), tile)
        return (
            pltpu.make_async_copy(new_ref.at[cut, :], new_hbm.at[cut, :], sems.at[0, i]),
            pltpu.make_async_copy(update_ref.at[cut, :], update_hbm.at[cut, :], sems.at[1, i]),
        )

    @pl.loop(0, steps)
    def _(i):
        cut = pl.ds(pl.multiple_of(i * tile, tile), tile)
        expanded = jnp.dot(p_ref[cut, :], whole[...], preferred_element_type=jnp.float32)
        new_ref[cut, :] = w_ref[cut, :] - step_rate * expanded
        update_ref[cut, :] = expanded.astype(update_ref.dtype)
        for copy in copies(i):
            copy.start()

    @pl.loop(0, steps)
    def _(i):
        for copy in copies(i):
            copy.wait()


def expand(projector, weight, pieces, rows):
    depth, rank = projector.shape
    width = weight.shape[1]
    steps, f = 8, len(pieces)
    return pl.pallas_call(
        functools.partial(expand_kernel, f, rows),
        out_shape=[
            jax.ShapeDtypeStruct(weight.shape, jnp.float32),
            jax.ShapeDtypeStruct(weight.shape, jnp.bfloat16),
        ],
        in_specs=[pl.BlockSpec(memory_space=pltpu.VMEM)] * (2 + f),
        out_specs=[pl.BlockSpec(memory_space=pltpu.HBM)] * 2,
        scratch_shapes=[
            pltpu.VMEM((rank, width), jnp.bfloat16),
            pltpu.VMEM(weight.shape, jnp.float32),
            pltpu.VMEM(weight.shape, jnp.bfloat16),
            pltpu.SemaphoreType.DMA((2, steps)),
        ],
        compiler_params=pltpu.CompilerParams(vmem_limit_bytes=20 << 20),
        cost_estimate=pl.CostEstimate(
            flops=2 * depth * rank * width,
            bytes_accessed=10 * depth * width + 2 * rank * (depth + width),
            transcendentals=0,
        ),
        name="expand",
    )(projector, weight, *pieces)


def local(ndp, nmp, activations, out_grads, projector, weight, first_moment, second_moment):
    rows, columns = first_moment.shape
    first, *rest = stages(ndp)
    pair = first[1]
    sends, projector, turned, grads = front(activations, out_grads, projector, ndp, pair, rows)
    got = exchange(sends, "dp", ndp, *first)
    kept = keep(turned, grads, pair, rows)
    crossed = pair == 2 and rest == [(pair, nmp)]
    if crossed:
        early, late = EARLY, 1 - EARLY
        kept, sends = cross_split(kept, got, nmp, pair, early, rows, columns)
        weight = load(weight, kept)
        got = cross(sends, ndp, nmp, pair, early, SUMS[0])
        got, weight = lax.optimization_barrier((got, weight))
        kept, sends = second_split(kept, got, nmp, pair, early, rows)
        got = cross(sends, ndp, nmp, pair, late, SUMS[1])
    else:
        for i, (stride, f) in enumerate(rest):
            kept, sends = split_rows(kept, got, "dp", stride, f, rows)
            if i == 0:
                weight = load(weight, kept)
            got = exchange(sends, "dp", ndp, stride, f)
            if i == 0:
                got, weight = lax.optimization_barrier((got, weight))
        kept, sends = split_columns(kept, got, "mp", nmp)
        got = exchange(sends, "mp", nmp, 1, nmp)
    first_new, second_new = new_moments(kept, got, first_moment, second_moment)
    x = normalize(kept, got, first_moment, second_moment)
    if crossed:
        x = first_join(x, cross([x] * (nmp - 1), ndp, nmp, pair, late, GATHERS[0]), nmp, pair, early)
        x = cross_join(x, cross([x] * (nmp - 1), ndp, nmp, pair, early, GATHERS[1]), nmp, pair, early, rows)
    else:
        x = join_columns(x, exchange([x] * (nmp - 1), "mp", nmp, 1, nmp), "mp", nmp)
        for stride, f in reversed(rest):
            x = join_rows(x, exchange([x] * (f - 1), "dp", ndp, stride, f), "dp", stride, f, rows)
    pieces = [x] + exchange([x] * (pair - 1), "dp", ndp, *first)
    new_weight, update = expand(projector, weight, pieces, rows)
    return (new_weight, update, first_new, second_new)


def solution(mesh):
    ndp, nmp = mesh.shape["dp"], mesh.shape["mp"]
    in_specs = (
        P("dp", "mp"),
        P("dp", None),
        P("mp", None),
        P("mp", None),
        P("dp", "mp"),
        P("dp", "mp"),
    )
    out_specs = (P("mp", None), P("mp", None), P("dp", "mp"), P("dp", "mp"))

    def step(*args):
        return local(ndp, nmp, *args)

    return jax.shard_map(step, mesh=mesh, in_specs=in_specs, out_specs=out_specs, check_vma=False)
```

```python
import functools
import math

import jax
import jax.numpy as jnp
from jax import lax
from jax.experimental import pallas as pl
from jax.experimental.pallas import tpu as pltpu
from jax.sharding import PartitionSpec as P


first_decay = 0.9
second_decay = 0.999
first_bias = 1.0 - 0.9**2
second_bias = 1.0 - 0.999**2
epsilon = 1e-08
EARLY = 0
SUMS = (((3, 1, 2), (1, 2, 3)), ((1, 2, 3), (3, 2, 1)))
GATHERS = (((1, 2, 3), (1, 2, 3)), ((2, 1, 3), (1, 3, 2)))
step_rate = 0.00025


def stages(n):
    out, stride = [], 1
    while stride < n:
        left = n // stride
        if stride == 1 and left % 2 == 0:
            f = 2
        elif left % 4 == 0:
            f = 4
        elif left % 2 == 0:
            f = 2
        else:
            f = left
        out.append((stride, f))
        stride *= f
    return out


def other(d, k, f):
    if f & (f - 1) == 0:
        return d ^ k, d ^ k
    return (d + k) % f, (d - k + f) % f


def shift(x, axis, n, stride, f, k):
    pairs = []
    for i in range(n):
        d = (i // stride) % f
        pairs.append((i, i + (other(d, k, f)[0] - d) * stride))
    return lax.ppermute(x, axis, pairs)


def fits(*shapes):
    size = sum(math.prod(x.shape) * x.dtype.itemsize for x in shapes)
    return pltpu.CompilerParams(vmem_limit_bytes=int(size) + (1 << 20))


def on_chip(kernel, out, *args, flops=0):
    vmem = pl.BlockSpec(memory_space=pltpu.VMEM)
    size = sum(math.prod(x.shape) * x.dtype.itemsize for x in [*args, *out])
    return pl.pallas_call(
        kernel,
        out_shape=[pltpu.VMEM(x.shape, x.dtype) for x in out],
        in_specs=[vmem] * len(args),
        out_specs=[vmem] * len(out),
        compiler_params=fits(*args, *out),
        cost_estimate=pl.CostEstimate(flops=flops, bytes_accessed=size, transcendentals=0),
    )(*args)


def exchange(sends, axis, n, stride, f):
    return [shift(x, axis, n, stride, f, k + 1) for k, x in enumerate(sends)]


def digit(axis, stride, f):
    return (lax.axis_index(axis) // stride) % f


def total_of(kept, got, *at):
    x = kept[at]
    for g in got:
        x = x + g[at].astype(jnp.float32)
    return x


def split_rows_kernel(axis, stride, f, rows, count, *refs):
    kept, got, out = refs[0], refs[1:count], refs[count:]
    d = digit(axis, stride, f)
    for k in range(f):
        for h in range(out[k].shape[0] // rows):
            at = pl.multiple_of((h * f + other(d, k, f)[0]) * rows, rows)
            x = total_of(kept, got, pl.ds(at, rows), slice(None))
            out[k][pl.ds(h * rows, rows), :] = x.astype(out[k].dtype)


def split_columns_kernel(axis, f, count, *refs):
    kept, got, out = refs[0], refs[1:count], refs[count:]
    d, width = digit(axis, 1, f), out[0].shape[1]
    for k in range(f):
        at = pl.multiple_of(other(d, k, f)[0] * width, width)
        out[k][...] = total_of(kept, got, slice(None), pl.ds(at, width)).astype(out[k].dtype)


def parts(shape, f):
    wide, narrow = jax.ShapeDtypeStruct(shape, jnp.float32), jax.ShapeDtypeStruct(shape, jnp.bfloat16)
    return [wide] + [narrow] * (f - 1)


def split_rows(kept, got, axis, stride, f, rows):
    kernel = functools.partial(split_rows_kernel, axis, stride, f, rows, 1 + len(got))
    out = parts((kept.shape[0] // f, kept.shape[1]), f)
    kept, *sends = on_chip(kernel, out, kept, *got)
    return kept, sends


def split_columns(kept, got, axis, f):
    kernel = functools.partial(split_columns_kernel, axis, f, 1 + len(got))
    out = parts((kept.shape[0], kept.shape[1] // f), f)
    kept, *sends = on_chip(kernel, out, kept, *got)
    return kept, sends


def turns(nmp, stride, first):
    f = nmp
    along_dp = lax.axis_index("dp") % stride == first
    q, z = digit("dp", stride, f), digit("mp", 1, f)
    return along_dp, lax.select(along_dp, q, z), lax.select(along_dp, z, q)


def distances(orders, i, f):
    if i == 0 or f != 4:
        return i, i
    return orders[0][i - 1], orders[1][i - 1]


def partner(orders, i, f, along_dp, mine, way):
    p, m = distances(orders, i, f)
    return lax.select(along_dp, other(mine, p, f)[way], other(mine, m, f)[way])


def cross(sends, ndp, nmp, stride, early, orders):
    got = []
    for i, x in enumerate(sends, 1):
        p, m = distances(orders, i, nmp)
        pairs = []
        for dp in range(ndp):
            for mp in range(nmp):
                q = (dp // stride) % nmp
                if dp % stride == early:
                    to = (dp + (other(q, p, nmp)[0] - q) * stride) * nmp + mp
                else:
                    to = dp * nmp + other(mp, m, nmp)[0]
                pairs.append((dp * nmp + mp, to))
        got.append(lax.ppermute(x, ("dp", "mp"), pairs))
    return got


def cross_split_kernel(f, stride, first, rows, width, count, *refs):
    kept, got, out = refs[0], refs[1:count], refs[count:]
    along_dp, mine, _ = turns(f, stride, first)
    for k in range(f):
        d = partner(SUMS[0], k, f, along_dp, mine, 0)
        for o in range(f):
            h, j = lax.select(along_dp, d, o), lax.select(along_dp, o, d)
            at = pl.ds(pl.multiple_of(h * rows, rows), rows), pl.ds(pl.multiple_of(j * width, width), width)
            out[k][pl.ds(o * rows, rows), :] = total_of(kept, got, *at).astype(out[k].dtype)


def cross_split(kept, got, f, stride, first, rows, width):
    kernel = functools.partial(cross_split_kernel, f, stride, first, rows, width, 1 + len(got))
    kept, *sends = on_chip(kernel, parts((f * rows, width), f), kept, *got)
    return kept, sends


def second_split_kernel(f, stride, first, rows, count, *refs):
    kept, got, out = refs[0], refs[1:count], refs[count:]
    along_dp, _, mine = turns(f, stride, first)
    for k in range(f):
        d = partner(SUMS[1], k, f, jnp.logical_not(along_dp), mine, 0)
        at = pl.multiple_of(d * rows, rows)
        out[k][...] = total_of(kept, got, pl.ds(at, rows), slice(None)).astype(out[k].dtype)


def second_split(kept, got, f, stride, first, rows):
    kernel = functools.partial(second_split_kernel, f, stride, first, rows, 1 + len(got))
    kept, *sends = on_chip(kernel, parts((rows, kept.shape[1]), f), kept, *got)
    return kept, sends


def first_join_kernel(f, stride, first, rows, *refs):
    out, (along_dp, _, mine) = refs[-1], turns(f, stride, first)
    for k in range(f):
        d = partner(GATHERS[0], k, f, jnp.logical_not(along_dp), mine, 1)
        at = pl.multiple_of(d * rows, rows)
        out[pl.ds(at, rows), :] = refs[k][...]


def first_join(x, got, f, stride, first):
    rows, width = x.shape
    kernel = functools.partial(first_join_kernel, f, stride, first, rows)
    out = [jax.ShapeDtypeStruct((f * rows, width), x.dtype)]
    return on_chip(kernel, out, x, *got)[0]


def stack_kernel(*refs):
    out, size = refs[-1], refs[0].shape[0]
    for i, ref in enumerate(refs[:-1]):
        out[pl.ds(i * size, size), :] = ref[...]


def stack(blocks):
    out = [jax.ShapeDtypeStruct((len(blocks) * blocks[0].shape[0], blocks[0].shape[1]), blocks[0].dtype)]
    return on_chip(stack_kernel, out, *blocks)[0]


def cross_join_kernel(f, stride, first, rows, *refs):
    own, (many, one, out) = refs[:f], refs[f:]
    width, size = own[0].shape[1], own[0].shape[0]
    along, (q, z) = turns(f, stride, first)[0], (digit("dp", stride, f), digit("mp", 1, f))
    c = digit("dp", 1, stride)
    for theirs in (False, True):
        along_dp = jnp.logical_not(along) if theirs else along
        mine = lax.select(along_dp, q, z)
        for k in range(f):
            d = partner(GATHERS[1], k, f, along_dp, mine, 1)
            if not theirs:
                ref, base = own[k], 0
            else:
                ref, base = (one, 0) if k == 1 else (many, [0, None, *range(1, f)][k] * size)
            for o in range(f):
                h, j = lax.select(along_dp, d, o), lax.select(along_dp, o, d)
                row = h * stride + (stride - 1 - c if theirs else c)
                at = pl.ds(pl.multiple_of(row * rows, rows), rows), pl.ds(pl.multiple_of(j * width, width), width)
                out[at] = ref[pl.ds(base + o * rows, rows), :]


def moments(count, refs):
    c = total_of(refs[0], refs[1:count], slice(None), slice(None))
    first_ref, second_ref = refs[count], refs[count + 1]
    first_new = first_decay * first_ref[...] + (1.0 - first_decay) * c
    second_new = second_decay * second_ref[...] + (1.0 - second_decay) * c * c
    return first_new, second_new


def normalize_kernel(count, *refs):
    first_new, second_new = moments(count, refs)
    x = first_new / first_bias / (jnp.sqrt(second_new / second_bias) + epsilon)
    refs[-1][...] = x.astype(refs[-1].dtype)


def moments_kernel(count, *refs):
    refs[-2][...], refs[-1][...] = moments(count, refs)


def normalize(kept, got, first_moment, second_moment):
    kernel = functools.partial(normalize_kernel, 1 + len(got))
    out = [jax.ShapeDtypeStruct(kept.shape, jnp.bfloat16)]
    return on_chip(kernel, out, kept, *got, first_moment, second_moment)[0]


def new_moments(kept, got, first_moment, second_moment):
    args = [kept, *got, first_moment, second_moment]
    out = [jax.ShapeDtypeStruct(kept.shape, jnp.float32)] * 2
    return pl.pallas_call(
        functools.partial(moments_kernel, 1 + len(got)),
        out_shape=out,
        compiler_params=fits(*args, *out),
        cost_estimate=pl.CostEstimate(flops=1 << 28, bytes_accessed=16 * kept.size, transcendentals=0),
        name="new_moments",
    )(*args)


def join_columns_kernel(axis, f, *refs):
    out, d, width = refs[-1], digit(axis, 1, f), refs[0].shape[1]
    for k in range(f):
        at = pl.multiple_of(other(d, k, f)[1] * width, width)
        out[:, pl.ds(at, width)] = refs[k][...]


def join_columns(x, got, axis, f):
    out = [jax.ShapeDtypeStruct((x.shape[0], x.shape[1] * f), x.dtype)]
    kernel = functools.partial(join_columns_kernel, axis, f)
    return on_chip(kernel, out, x, *got)[0]


def join_rows_kernel(axis, stride, f, rows, *refs):
    out, d = refs[-1], digit(axis, stride, f)
    for k in range(f):
        for h in range(refs[k].shape[0] // rows):
            at = pl.multiple_of((h * f + other(d, k, f)[1]) * rows, rows)
            out[pl.ds(at, rows), :] = refs[k][pl.ds(h * rows, rows), :]


def join_rows(x, got, axis, stride, f, rows):
    out = [jax.ShapeDtypeStruct((x.shape[0] * f, x.shape[1]), x.dtype)]
    kernel = functools.partial(join_rows_kernel, axis, stride, f, rows)
    return on_chip(kernel, out, x, *got)[0]


def in_vmem(shape, dtype):
    return pltpu.VMEM(shape, dtype)


def front_kernel(f, rows, a_hbm, p_hbm, g_hbm, *refs):
    send_refs, (p_ref, turned, g_ref, a_ref, total, picked, sems) = refs[: f - 1], refs[f - 1 :]
    depth = a_ref.shape[1]
    steps = sems.shape[1]
    tile = depth // steps
    copies = []
    for i in range(steps):
        cut = pl.ds(i * tile, tile)
        copies.append(
            (
                pltpu.make_async_copy(a_hbm.at[:, cut], a_ref.at[:, cut], sems.at[0, i]),
                pltpu.make_async_copy(p_hbm.at[cut, :], p_ref.at[cut, :], sems.at[1, i]),
            )
        )
    late = pltpu.make_async_copy(g_hbm, g_ref, sems.at[2, 0])
    for pair in copies:
        for copy in pair:
            copy.start()
    late.start()
    for i, pair in enumerate(copies):
        for copy in pair:
            copy.wait()
        cut = pl.ds(i * tile, tile)
        part = jnp.dot(a_ref[:, cut], p_ref[cut, :], preferred_element_type=jnp.float32)
        total[...] = part if i == 0 else total[...] + part
    turned[...] = total[...].astype(turned.dtype).T
    late.wait()
    half_kernel(f, rows, range(1, f), turned, g_ref, picked, send_refs)


def half_kernel(f, rows, which, turned, g_ref, picked, out):
    mine = digit("dp", 1, f)
    for k, ref in zip(which, out):
        d = other(mine, k, f)[0]
        for h in range(picked.shape[0] // rows):
            at = pl.multiple_of((h * f + d) * rows, rows)
            picked[pl.ds(h * rows, rows), :] = turned[pl.ds(at, rows), :]
        part = jnp.dot(picked[...], g_ref[...], preferred_element_type=jnp.float32)
        ref[...] = part.astype(ref.dtype)


def keep_kernel(f, rows, turned, g_ref, keep_ref, picked):
    half_kernel(f, rows, [0], turned, g_ref, picked, [keep_ref])


def keep(turned, out_grads, f, rows):
    rank, tokens = turned.shape
    width = out_grads.shape[1]
    out = jax.ShapeDtypeStruct((rank // f, width), jnp.float32)
    return pl.pallas_call(
        functools.partial(keep_kernel, f, rows),
        out_shape=pltpu.VMEM(out.shape, out.dtype),
        in_specs=[pl.BlockSpec(memory_space=pltpu.VMEM)] * 2,
        out_specs=pl.BlockSpec(memory_space=pltpu.VMEM),
        scratch_shapes=[pltpu.VMEM((rank // f, tokens), jnp.bfloat16)],
        compiler_params=fits(turned, out_grads, out),
        cost_estimate=pl.CostEstimate(
            flops=2 * tokens * rank * width // f, bytes_accessed=4 * out.size, transcendentals=0
        ),
        name="keep",
    )(turned, out_grads)


def front(activations, out_grads, projector, f, rows):
    tokens, depth = activations.shape
    rank, width = projector.shape[1], out_grads.shape[1]
    part = rank // f
    hbm = pl.BlockSpec(memory_space=pltpu.HBM)
    vmem = pl.BlockSpec(memory_space=pltpu.VMEM)
    *sends, copy, turned, grads = pl.pallas_call(
        functools.partial(front_kernel, f, rows),
        out_shape=[in_vmem((part, width), jnp.bfloat16)] * (f - 1)
        + [
            in_vmem(projector.shape, projector.dtype),
            in_vmem((rank, tokens), jnp.bfloat16),
            in_vmem(out_grads.shape, out_grads.dtype),
        ],
        in_specs=[hbm] * 3,
        out_specs=[vmem] * (f + 2),
        scratch_shapes=[
            pltpu.VMEM((tokens, depth), jnp.bfloat16),
            pltpu.VMEM((tokens, rank), jnp.float32),
            pltpu.VMEM((part, tokens), jnp.bfloat16),
            pltpu.SemaphoreType.DMA((3, 4)),
        ],
        compiler_params=pltpu.CompilerParams(vmem_limit_bytes=16 << 20),
        cost_estimate=pl.CostEstimate(
            flops=2 * tokens * rank * (depth + width),
            bytes_accessed=2 * (tokens * depth + depth * rank + tokens * width),
            transcendentals=0,
        ),
        name="front",
    )(
        pltpu.with_memory_space_constraint(activations, pltpu.HBM),
        pltpu.with_memory_space_constraint(projector, pltpu.HBM),
        pltpu.with_memory_space_constraint(out_grads, pltpu.HBM),
    )
    return sends, copy, turned, grads


def load_kernel(w_hbm, after_ref, w_ref, sem):
    copy = pltpu.make_async_copy(w_hbm, w_ref, sem)
    copy.start()
    copy.wait()


def load(weight, after):
    return pl.pallas_call(
        load_kernel,
        out_shape=in_vmem(weight.shape, weight.dtype),
        in_specs=[pl.BlockSpec(memory_space=pltpu.HBM), pl.BlockSpec(memory_space=pl.ANY)],
        out_specs=pl.BlockSpec(memory_space=pltpu.VMEM),
        scratch_shapes=[pltpu.SemaphoreType.DMA],
        compiler_params=pltpu.CompilerParams(vmem_limit_bytes=1 << 20),
        cost_estimate=pl.CostEstimate(
            flops=600 * weight.size, bytes_accessed=4 * weight.size, transcendentals=0
        ),
        name="load",
    )(pltpu.with_memory_space_constraint(weight, pltpu.HBM), after)


def expand_kernel(join, count, p_ref, w_ref, *refs):
    pieces, (new_hbm, update_hbm, whole, new_ref, update_ref, sems) = refs[:count], refs[count:]
    join(*pieces, whole)
    steps = sems.shape[1]
    tile = w_ref.shape[0] // steps

    def copies(i):
        cut = pl.ds(pl.multiple_of(i * tile, tile), tile)
        return (
            pltpu.make_async_copy(new_ref.at[cut, :], new_hbm.at[cut, :], sems.at[0, i]),
            pltpu.make_async_copy(update_ref.at[cut, :], update_hbm.at[cut, :], sems.at[1, i]),
        )

    @pl.loop(0, steps)
    def _(i):
        cut = pl.ds(pl.multiple_of(i * tile, tile), tile)
        expanded = jnp.dot(p_ref[cut, :], whole[...], preferred_element_type=jnp.float32)
        new_ref[cut, :] = w_ref[cut, :] - step_rate * expanded
        update_ref[cut, :] = expanded.astype(update_ref.dtype)
        for copy in copies(i):
            copy.start()

    @pl.loop(0, steps)
    def _(i):
        for copy in copies(i):
            copy.wait()


def expand(projector, weight, pieces, join):
    depth, rank = projector.shape
    width = weight.shape[1]
    steps, f = 8, len(pieces)
    return pl.pallas_call(
        functools.partial(expand_kernel, join, f),
        out_shape=[
            jax.ShapeDtypeStruct(weight.shape, jnp.float32),
            jax.ShapeDtypeStruct(weight.shape, jnp.bfloat16),
        ],
        in_specs=[pl.BlockSpec(memory_space=pltpu.VMEM)] * (2 + f),
        out_specs=[pl.BlockSpec(memory_space=pltpu.HBM)] * 2,
        scratch_shapes=[
            pltpu.VMEM((rank, width), jnp.bfloat16),
            pltpu.VMEM(weight.shape, jnp.float32),
            pltpu.VMEM(weight.shape, jnp.bfloat16),
            pltpu.SemaphoreType.DMA((2, steps)),
        ],
        compiler_params=pltpu.CompilerParams(vmem_limit_bytes=20 << 20),
        cost_estimate=pl.CostEstimate(
            flops=2 * depth * rank * width,
            bytes_accessed=10 * depth * width + 2 * rank * (depth + width),
            transcendentals=0,
        ),
        name="expand",
    )(projector, weight, *pieces)


def local(ndp, nmp, activations, out_grads, projector, weight, first_moment, second_moment):
    rows, columns = first_moment.shape
    first, *rest = stages(ndp)
    pair = first[1]
    sends, projector, turned, grads = front(activations, out_grads, projector, pair, rows)
    got = exchange(sends, "dp", ndp, *first)
    kept = keep(turned, grads, pair, rows)
    crossed = pair == 2 and rest == [(pair, nmp)]
    if crossed:
        early, late = EARLY, 1 - EARLY
        kept, sends = cross_split(kept, got, nmp, pair, early, rows, columns)
        weight = load(weight, kept)
        got = cross(sends, ndp, nmp, pair, early, SUMS[0])
        got, weight = lax.optimization_barrier((got, weight))
        kept, sends = second_split(kept, got, nmp, pair, early, rows)
        got = cross(sends, ndp, nmp, pair, late, SUMS[1])
    else:
        for i, (stride, f) in enumerate(rest):
            kept, sends = split_rows(kept, got, "dp", stride, f, rows)
            if i == 0:
                weight = load(weight, kept)
            got = exchange(sends, "dp", ndp, stride, f)
            if i == 0:
                got, weight = lax.optimization_barrier((got, weight))
        kept, sends = split_columns(kept, got, "mp", nmp)
        got = exchange(sends, "mp", nmp, 1, nmp)
    first_new, second_new = new_moments(kept, got, first_moment, second_moment)
    x = normalize(kept, got, first_moment, second_moment)
    if crossed:
        x = first_join(x, cross([x] * (nmp - 1), ndp, nmp, pair, late, GATHERS[0]), nmp, pair, early)
        got = cross([x] * (nmp - 1), ndp, nmp, pair, early, GATHERS[1])
        (many,) = exchange([stack([x, *got[1:]])], "dp", ndp, *first)
        (one,) = exchange([got[0]], "dp", ndp, *first)
        pieces = [x, *got, many, one]
        join = functools.partial(cross_join_kernel, nmp, pair, early, rows)
    else:
        x = join_columns(x, exchange([x] * (nmp - 1), "mp", nmp, 1, nmp), "mp", nmp)
        for stride, f in reversed(rest):
            x = join_rows(x, exchange([x] * (f - 1), "dp", ndp, stride, f), "dp", stride, f, rows)
        pieces = [x] + exchange([x] * (pair - 1), "dp", ndp, *first)
        join = functools.partial(join_rows_kernel, "dp", 1, pair, rows)
    new_weight, update = expand(projector, weight, pieces, join)
    return (new_weight, update, first_new, second_new)


def solution(mesh):
    ndp, nmp = mesh.shape["dp"], mesh.shape["mp"]
    in_specs = (
        P("dp", "mp"),
        P("dp", None),
        P("mp", None),
        P("mp", None),
        P("dp", "mp"),
        P("dp", "mp"),
    )
    out_specs = (P("mp", None), P("mp", None), P("dp", "mp"), P("dp", "mp"))

    def step(*args):
        return local(ndp, nmp, *args)

    step = jax.shard_map(step, mesh=mesh, in_specs=in_specs, out_specs=out_specs, check_vma=False)
    return step
```
